32 devices in a mesh: grp: 4 (over y, x), row: 8 (over z, core).
Axes of the slice: x: 2, y: 2, z: 4, core: 2. Of those that a mesh axis runs over, the one named last changes fastest.
Arguments:
- serving: bfloat16 [16384, 128], P('row'), may hold values from -1 to 1
- serving_scale: bfloat16 [128], P('row'), may hold values from 0.099609375 to 1
- hot_blocks: int32 [4, 16], P('grp', 'row'), may hold values from 0 to 15, as said below
- bag_lengths: int32 [32, 256], P(('grp', 'row')), may hold values from 1 to 16, 1024 in all within a row
- bag_indices: int32 [32, 1024], P(('grp', 'row')), may hold values from 0 to 2047, as said below
- dense_act: bfloat16 [8192, 128], P(('grp', 'row')), may hold values from -6 to 6
- labels: float32 [8192], P(('grp', 'row')), may hold values from 0 to 1
- w_top: bfloat16 [256, 1024], replicated, may hold values from -0.375 to 0.375
- w_out: float32 [1024], replicated, may hold values from -0.012 to 0.012
- master: float32 [4, 4096, 128], P('grp', 'row'), may hold values from -0.3 to 0.3
- accum: float32 [4, 4096], P('grp', 'row'), may hold values from 1e-05 to 0.0001
Outputs:
- new_master: float32 [4, 4096, 128], P('grp', 'row')
- new_accum: float32 [4, 4096], P('grp', 'row')
- new_serving: bfloat16 [16384, 128], P('row')
- new_scale: bfloat16 [128], P('row')
- top_grad: float32 [256, 1024], replicated
The draws below stay inside these ranges and needn't reach their ends.
Inputs may be any that keep to these rules, and one draw needn't show every extreme that they name: `hot_blocks`: the 2 entries that one group names in one row shard are distinct. `bag_indices`: in each device's line, exactly 64 distinct values lie in each range of 256 consecutive positions that starts at a multiple of 256.
All inputs are finite; a program needn't handle non-finite values. Where the reference program divides by a largest or mean magnitude, that divisor is 1e-20 or more.
Results may differ from the reference program's by a relative error of at most 0.012.
Values may be sent and summed in bfloat16 or wider, within the bound.
A program may use at most 128 MiB of HBM per device.

```python
import math
import jax
import jax.numpy as jnp
import numpy as np
from jax import lax

D = 128
DENSE_W = 128
FF = 1024
BLOCK = 128
BLK_DEV = 16
HOT_DEV = 2
BAGS_DEV = 256
MOST = 16
NNZ_DEV = 1024
CAP = 64
ROWS = 16384
HOTROWS = 2048
BAGS = 8192
N_GRP = 4
N_ROW = 8
DEVICES = 32


def draw_hot_blocks(key, part):
    keys = jax.random.split(jax.random.fold_in(key, 11), N_GRP * N_ROW)
    picks = jax.vmap(lambda one: jax.random.permutation(one, BLK_DEV)[:HOT_DEV])(keys)
    return picks.reshape(N_GRP, N_ROW * HOT_DEV).astype(jnp.int32)


def draw_bag_indices(key, part):
    span = HOT_DEV * BLOCK
    base = N_ROW * CAP

    def one_device(device_key):
        keys = jax.random.split(device_key, N_ROW + 4)
        picks = jax.vmap(lambda one: jax.random.permutation(one, span)[:CAP])(keys[:N_ROW])
        offsets = (jnp.arange(N_ROW, dtype=jnp.int32) * span)[:, None]
        candidates = (picks.astype(jnp.int32) + offsets).reshape(base)
        candidates = jax.random.permutation(keys[N_ROW], candidates)
        first_pick = jax.random.randint(keys[N_ROW + 1], (NNZ_DEV - base,), 0, base)
        second_pick = jax.random.randint(keys[N_ROW + 2], (NNZ_DEV - base,), 0, base)
        repeats = candidates[jnp.minimum(first_pick, second_pick)]
        return jax.random.permutation(keys[N_ROW + 3], jnp.concatenate([candidates, repeats])).astype(jnp.int32)
    device_keys = jax.random.split(jax.random.fold_in(key, 23), DEVICES)
    return jax.vmap(one_device)(device_keys)


def level_of(rng, extent, cuts, smallest, largest):
    def one(axis_at, shards_of):
        draws = jax.random.uniform(jax.random.fold_in(jax.random.fold_in(rng, 6), axis_at), (shards_of,), jnp.float32, smallest / len(cuts), largest / len(cuts))
        return jnp.repeat(jnp.exp(draws), extent[axis_at] // shards_of).reshape((-1,) + (1,) * (len(extent) - axis_at - 1))

    level = one(*cuts[0])
    for cut in cuts[1:]:
        level = level * one(*cut)
    return level


def split_up(number_of, total, bound, lean):
    portions = [(1 << 20) // math.isqrt(rank ** lean) + 1 for rank in range(2, number_of + 1)]
    surplus, counts = total - bound - (number_of - 1), [1] * (number_of - 1)
    while surplus > 0:
        movable = [i for i in range(number_of - 1) if counts[i] < bound]
        pool, left = sum([portions[i] for i in movable]), surplus
        for i in movable:
            more = min(bound - counts[i], max(1, left * portions[i] // pool), surplus)
            counts[i] = counts[i] + more
            surplus = surplus - more
    return np.array([bound] + counts)


def ragged(key, number_of, total, reach, skew):
    if number_of == 2:
        one = jax.random.randint(key, (), max(1, total - reach), min(reach, total - 1) + 1)
        return jnp.stack([one, total - one])
    tallies = jnp.asarray(split_up(number_of, total, reach, skew), jnp.int32)
    twos = (number_of - 1) // 2
    giver, sink = tallies[1:1 + 2 * twos:2], tallies[2:2 + 2 * twos:2]
    slack = jnp.minimum(giver - 1, reach - sink)
    moved = jax.random.randint(jax.random.fold_in(key, 1), (twos,), 0, 1 << 20) % (slack + 1)
    tallies = tallies.at[1:1 + 2 * twos:2].set(giver - moved).at[2:2 + 2 * twos:2].set(sink + moved)
    return tallies[jax.random.permutation(jax.random.fold_in(key, 2), number_of)]


def centred(rng, extent, spread, most, cuts=(), kind=jnp.bfloat16):
    level = level_of(rng, extent, cuts, -0.22, 0.18) if cuts else 1.0
    result = jax.random.normal(rng, extent, jnp.float32) * spread * level
    return jnp.minimum(jnp.maximum(result, -most), most).astype(kind)


def setup_inputs(seed: int = 0) -> dict:
    key_list = jax.random.split(jax.random.key(seed), 12)
    serving = jnp.clip(jax.random.uniform(key_list[0], (ROWS, D), jnp.float32, -1.0, 1.0) * level_of(key_list[0], (ROWS, D), ((0, 8),), -0.4, 0.0), -1.0, 1.0).astype(jnp.bfloat16)
    serving_scale = jnp.clip(jnp.exp(math.log(1.0) - 2.306499 * jax.random.uniform(key_list[1], (ROWS // BLOCK,), jnp.float32) ** level_of(key_list[1], (ROWS // BLOCK,), ((0, 8),), -0.2, 0.2)), 0.099609375, 1.0).astype(jnp.bfloat16)
    hot_blocks = draw_hot_blocks(jax.random.fold_in(key_list[11], 71), 0)
    bag_lengths = jax.vmap(lambda own: ragged(own, BAGS_DEV, NNZ_DEV, MOST, 1))(jax.random.split(key_list[3], DEVICES)).reshape((DEVICES, BAGS_DEV)).astype(jnp.int32)
    bag_indices = draw_bag_indices(jax.random.fold_in(key_list[11], 71), 0)
    dense_act = centred(key_list[5], (BAGS, DENSE_W), 1.0, 6.0, ((0, 32),))
    labels = jnp.clip(1.0 * jax.random.uniform(key_list[6], (BAGS,), jnp.float32) ** level_of(key_list[6], (BAGS,), ((0, 32),), -0.2, 0.2), 0.0, 1.0)
    w_top = centred(key_list[7], (D + DENSE_W, FF), (D + DENSE_W) ** -0.5, 0.375)
    w_out = centred(key_list[8], (FF,), 0.002, 0.012, (), jnp.float32)
    master = centred(key_list[9], (N_GRP, ROWS // N_GRP, D), 0.05, 0.3, ((0, 4), (1, 8)), jnp.float32)
    accum = jnp.clip(jnp.exp(math.log(0.0001) - 2.3025851 * jax.random.uniform(key_list[10], (N_GRP, ROWS // N_GRP), jnp.float32) ** level_of(key_list[10], (N_GRP, ROWS // N_GRP), ((0, 4), (1, 8)), -0.2, 0.2)), 9.999999747378752e-06, 0.0001)
    return {"serving": serving, "serving_scale": serving_scale, "hot_blocks": hot_blocks, "bag_lengths": bag_lengths, "bag_indices": bag_indices, "dense_act": dense_act, "labels": labels, "w_top": w_top, "w_out": w_out, "master": master, "accum": accum}


lr_step = 0.05

def pool_grad(table, lengths, indices, dense_d, labels_d, w_top, w_out):
    ends = jnp.cumsum(lengths).astype(jnp.int32)
    starts = ends - lengths
    marks = jnp.zeros((indices.shape[0],), jnp.int32).at[starts].add(1)
    bag = (jnp.cumsum(marks) - 1).astype(jnp.int32)
    pooled = jax.ops.segment_sum(table[indices], bag, num_segments=lengths.shape[0])
    joined = jnp.concatenate([pooled.astype(jnp.bfloat16), dense_d], axis=1)
    pre = jnp.dot(joined, w_top, preferred_element_type=jnp.float32)
    sig = jax.nn.sigmoid(pre)
    logit = jnp.dot(pre * sig, w_out, precision=lax.Precision.HIGHEST)
    dlogit = jax.nn.sigmoid(logit) - labels_d
    dpre = (dlogit[:, None] * w_out[None, :] * (sig * (1.0 + pre * (1.0 - sig)))).astype(jnp.bfloat16)
    top = lax.dot_general(joined, dpre, (((0,), (0,)), ((), ())), preferred_element_type=jnp.float32)
    dz = lax.dot_general(dpre, w_top, (((1,), (1,)), ((), ())), preferred_element_type=jnp.float32)
    width = table.shape[1]
    hot = jax.ops.segment_sum(dz[:, :width][bag], indices, num_segments=table.shape[0])
    return (top, hot)

def reference(serving, serving_scale, hot_blocks, bag_lengths, bag_indices, dense_act, labels, w_top, w_out, master, accum):
    span = BLK_DEV * BLOCK
    quarter = span // N_GRP
    shard_of = jnp.arange(N_ROW * HOT_DEV, dtype=jnp.int32) // HOT_DEV * BLK_DEV
    block_ids = (shard_of[None, :] + hot_blocks).astype(jnp.int32)
    blocks = serving.reshape(N_ROW * BLK_DEV, BLOCK, D)
    tables = (blocks[block_ids].astype(jnp.float32) * serving_scale[block_ids].astype(jnp.float32)[..., None, None]).reshape(N_GRP, HOTROWS, D)
    dense = dense_act.reshape(DEVICES, BAGS_DEV, DENSE_W)
    label_rows = labels.reshape(DEVICES, BAGS_DEV)

    def one_device(carry, xs):
        top_sum, hot_sums = carry
        device, lengths, indices, dense_d, labels_d = xs
        group = (device // N_ROW).astype(jnp.int32)
        table = lax.dynamic_index_in_dim(tables, group, 0, keepdims=False)
        top, hot = pool_grad(table, lengths, indices, dense_d, labels_d, w_top, w_out)
        old = lax.dynamic_index_in_dim(hot_sums, group, 0, keepdims=True)
        hot_sums = lax.dynamic_update_index_in_dim(hot_sums, old + hot[None], group, 0)
        return ((top_sum + top, hot_sums), None)
    start = (jnp.zeros((D + DENSE_W, FF), jnp.float32), jnp.zeros((N_GRP, HOTROWS, D), jnp.float32))
    xs = (jnp.arange(DEVICES, dtype=jnp.int32), bag_lengths, bag_indices, dense, label_rows)
    (top_grad, hot_sums), _ = lax.scan(one_device, start, xs)
    row_grad = jnp.zeros((N_ROW * BLK_DEV, BLOCK, D), jnp.float32).at[block_ids.reshape(-1)].add(hot_sums.reshape(N_GRP * N_ROW * HOT_DEV, BLOCK, D))
    row_grad = row_grad.reshape(ROWS, D)
    table_master = master.reshape(N_GRP, N_ROW, quarter, D).transpose(1, 0, 2, 3).reshape(ROWS, D)
    table_accum = accum.reshape(N_GRP, N_ROW, quarter).transpose(1, 0, 2).reshape(ROWS)
    new_state = table_accum + lax.optimization_barrier(jnp.mean(row_grad * row_grad, axis=1))
    new_weights = table_master - lr_step * row_grad / jnp.sqrt(new_state)[:, None]
    scale_new = (lax.optimization_barrier(jnp.max(jnp.abs(new_weights.reshape(ROWS // BLOCK, BLOCK * D)), axis=1)) + 1e-06).astype(jnp.bfloat16)
    coded = (new_weights.reshape(ROWS // BLOCK, BLOCK, D) / scale_new.astype(jnp.float32)[:, None, None]).astype(jnp.bfloat16).reshape(ROWS, D)
    out_master = new_weights.reshape(N_ROW, N_GRP, quarter, D).transpose(1, 0, 2, 3).reshape(N_GRP, ROWS // N_GRP, D)
    out_accum = new_state.reshape(N_ROW, N_GRP, quarter).transpose(1, 0, 2).reshape(N_GRP, ROWS // N_GRP)
    return (out_master, out_accum, coded, scale_new, top_grad)
```

```python
import functools

import jax
import jax.numpy as jnp
from jax import lax
from jax.experimental import pallas as pl
from jax.experimental.pallas import tpu as pltpu
from jax.sharding import PartitionSpec as P

BLOCK = 128
LR = 0.05
MESH = pl.DeviceIdType.MESH
BF = jnp.bfloat16
F32 = jnp.float32


def nt(a, b):
    return lax.dot_general(a, b, (((1,), (1,)), ((), ())), preferred_element_type=F32)


def nn(a, b):
    return jnp.dot(a, b, preferred_element_type=F32)


def tn(a, b):
    return lax.dot_general(a, b, (((0,), (0,)), ((), ())), preferred_element_type=F32)


def iota(shape, axis):
    return lax.broadcasted_iota(jnp.int32, shape, axis)


def to_column(row):
    m = row.shape[1]
    keep = iota((m, m), 0) == iota((m, m), 1)
    return jnp.sum(jnp.where(keep, row, jnp.zeros_like(row)), axis=1, keepdims=True)


def to_row(column):
    m = column.shape[0]
    keep = iota((m, m), 0) == iota((m, m), 1)
    return jnp.sum(jnp.where(keep, column, jnp.zeros_like(column)), axis=0, keepdims=True)


def rcopy(src, dst, send, recv, device):
    return pltpu.make_async_remote_copy(
        src_ref=src, dst_ref=dst, send_sem=send, recv_sem=recv,
        device_id=device, device_id_type=MESH,
    )


def loop(lo, hi, body):
    def step(k, carry):
        body(k)
        return carry

    lax.fori_loop(lo, hi, step, 0)


def kernel(
    dims,
    hot, srv, scl, lens, idx, dense, labels, w_top, w_out, master, accum,
    o_master, o_accum, o_srv, o_scl, o_top,
    tbl, cnt, cnt_t, sel, hmsg, hrecv, gbuf, sbuf, pooled, joined, dpre,
    t_send, t_own, t_a, t_b, t_br, t_c, t_cr, f_d, f_e, f_f,
    a_s, a_f, a_r, h_s, h_r, g_s, g_r, c_s, c_r, k_s, k_r,
    ta_s, ta_r, tb_s, tb_r, tc_s, tc_r, td_s, td_r, te_s, te_r, tf_s, tf_r,
):
    n, groups, cap = dims
    nz = n // 2
    g = lax.axis_index("grp")
    me = lax.axis_index("row")
    z, c = me // 2, me % 2
    pal = z * 2 + (1 - c)
    count = hot.shape[1]
    span = count * BLOCK
    capp = hmsg.shape[1] - 16
    bags = lens.shape[1]
    nnz = idx.shape[1]
    width = srv.shape[1]
    per = master.shape[0] // BLOCK
    ff = w_top.shape[1]
    half = ff // 2

    def row_peer(k):
        return (me + k) % n

    def chip_peer(k):
        return ((z + k) % nz) * 2 + c

    def grp_peer(k):
        return (g + k) % groups

    barrier = pltpu.get_barrier_semaphore()

    def greet(k):
        pl.semaphore_signal(barrier, inc=1, device_id=(g, row_peer(k)), device_id_type=MESH)

    loop(1, n, greet)
    for k in range(1, groups):
        pl.semaphore_signal(barrier, inc=1, device_id=(grp_peer(k), me), device_id_type=MESH)

    lane_b = iota((1, scl.shape[1]), 1)
    scales = scl[...].astype(F32)
    rows16 = iota((16, width), 0)
    scale_rows = jnp.zeros((16, width), F32)
    id_rows = jnp.zeros((16, width), F32)
    for j in range(count):
        block = hot[:, j:j + 1]
        one = jnp.sum(jnp.where(lane_b == block, scales, 0.0), axis=1, keepdims=True)
        scale_rows = jnp.where(rows16 == j, one, scale_rows)
        id_rows = jnp.where(rows16 == j, block.astype(F32), id_rows)
        chosen = jnp.broadcast_to(block, (8, width))
        rows = jnp.zeros((BLOCK, width), F32)
        for b in range(scl.shape[1]):
            mask = jnp.where(chosen == b, 1.0, 0.0)[0:1, :]
            rows = rows + srv[b * BLOCK:(b + 1) * BLOCK, :].astype(F32) * mask
        tbl[me, j * BLOCK:(j + 1) * BLOCK, :] = rows.astype(BF)
    tbl[me, span:span + 16, :] = scale_rows.astype(BF)
    gbuf[g, span:span + 16, :] = id_rows.astype(BF)

    pl.semaphore_wait(barrier, n - 1 + groups - 1)

    def a_copy(source, to, send):
        return rcopy(tbl.at[source], tbl.at[source], send, a_r.at[source], (g, to))

    loop(1, nz, lambda k: a_copy(me, chip_peer(k), a_s.at[k]).start())
    a_copy(me, pal, a_s.at[0]).start()

    lengths = lens[...]
    tri = iota((bags, bags), 1) <= iota((bags, bags), 0)
    ends = jnp.sum(jnp.where(tri, lengths, 0), axis=1, keepdims=True)
    starts = ends - to_column(lengths)
    place = iota((bags, nnz), 1)
    in_bag = jnp.where((place >= starts) & (place < ends), 1.0, 0.0).astype(BF)
    indices = idx[...]
    upper = jnp.where(iota((span, span), 0) <= iota((span, span), 1), 1.0, 0.0).astype(BF)
    numbers = iota((8, span), 1).astype(F32).astype(BF)

    def count_range(r):
        which = jnp.where(indices - r * span == iota((span, nnz), 0), 1.0, 0.0).astype(BF)
        cnt_t[r] = nt(which, in_bag).astype(BF)
        counts = nt(in_bag, which)
        cnt[r] = counts.astype(BF)
        used = jnp.where(jnp.sum(counts, axis=0, keepdims=True) > 0.0, 1.0, 0.0)
        rank = nn(jnp.broadcast_to(used, (8, span)).astype(BF), upper)[0:1, :]
        order = jnp.where(used > 0.0, rank.astype(jnp.int32) - 1, -1)
        picked = jnp.where(iota((width, span), 0) == order, 1.0, 0.0).astype(BF)
        sel[r] = picked[:capp, :]
        hmsg[r, capp:capp + 16, :] = jnp.concatenate(
            [nt(numbers, picked), jnp.zeros((8, width), F32)], axis=0
        ).astype(BF)

    loop(0, n, count_range)

    joined[:, width:] = dense[...]

    def relay(k):
        source = chip_peer(k)
        a_copy(source, source, a_f.at[k]).wait_recv()
        a_copy(source, pal, a_f.at[k]).start()

    loop(1, nz, relay)

    def other(k):
        source = ((z + k) % nz) * 2 + (1 - c)
        a_copy(source, pal, a_f.at[0]).wait_recv()

    loop(0, nz, other)
    pooled[...] = jnp.zeros_like(pooled)

    def pool(r):
        block_scale = tbl[r, span:span + 16, :].astype(F32)
        total = pooled[...]
        for j in range(count):
            part = slice(j * BLOCK, (j + 1) * BLOCK)
            total = total + nn(cnt[r, :, part], tbl[r, part, :]) * block_scale[j:j + 1, :]
        pooled[...] = total

    loop(0, n, pool)
    joined[:, :width] = pooled[...].astype(BF)

    pre = nn(joined[...], w_top[...])
    sig = jax.nn.sigmoid(pre)
    out_w = w_out[...]
    logit = jnp.sum(pre * sig * out_w, axis=1, keepdims=True)
    dlogit = jax.nn.sigmoid(logit) - to_column(labels[...])
    dp = (dlogit * out_w * (sig * (1.0 + pre * (1.0 - sig)))).astype(BF)
    dpre[0] = dp[:, :half]
    dpre[1] = dp[:, half:]
    dz = nt(dp, w_top[:width, :]).astype(BF)

    def h_copy(to, source, k):
        return rcopy(hmsg.at[to], hrecv.at[source], h_s.at[k], h_r.at[source], (g, to))

    def spread(k):
        to = row_peer(k)
        rows = nn(cnt_t[to], dz).astype(BF)
        hmsg[to, :capp, :] = nn(sel[to], rows).astype(BF)
        h_copy(to, me, k).start()

    loop(1, n, spread)

    def ta_copy():
        return rcopy(t_send, t_a, ta_s, ta_r, (g, pal))

    feats = w_top.shape[0]
    theirs = tn(joined[...], dpre[1 - c])
    for j in range(half // BLOCK):
        t_send[j * feats:(j + 1) * feats, :] = theirs[:, j * BLOCK:(j + 1) * BLOCK].astype(BF)
    ta_copy().start()
    mine = tn(joined[...], dpre[c])
    for j in range(half // BLOCK):
        t_own[j * feats:(j + 1) * feats, :] = mine[:, j * BLOCK:(j + 1) * BLOCK]

    pooled[...] = jnp.zeros_like(pooled)
    t_rows = nn(cnt_t[me], dz)

    def g_copy(k):
        return rcopy(gbuf.at[g], gbuf.at[g], g_s.at[k], g_r.at[k], (grp_peer(k), me))

    def arrive(k, total):
        source = row_peer(k)
        h_copy(source, source, k).wait_recv()
        place_of = hrecv[source, capp:capp + 1, :].astype(F32)
        put = jnp.where(
            iota((span, width), 0).astype(F32) == place_of, 1.0, 0.0
        ).astype(BF)
        return total + nn(put[:, :capp], hrecv[source, :capp, :])

    summed = lax.fori_loop(1, n, arrive, t_rows)
    gbuf[g, :span, :] = summed.astype(BF)
    for k in range(1, groups):
        g_copy(k).start()

    quarter = t_own.shape[0] // groups

    def part_of(ref, q):
        return ref.at[pl.ds(pl.multiple_of(q * quarter, quarter), quarter)]

    def tb_copy(k):
        return rcopy(
            part_of(t_b, grp_peer(k)), t_br.at[k], tb_s.at[k], tb_r.at[k], (grp_peer(k), me)
        )

    ta_copy().wait_recv()
    both = t_own[...] + t_a[...].astype(F32)
    t_own[...] = both
    t_b[...] = both.astype(BF)
    for k in range(1, groups):
        tb_copy(k).start()

    for k in range(1, groups):
        g_copy(k).wait_recv()
    srows = jnp.zeros((16, width), F32)
    quarter_at = (g * per).astype(F32)
    for b in range(per):
        grad = jnp.zeros((BLOCK, width), F32)
        for q in range(groups):
            for j in range(count):
                ids = gbuf[q, span:span + 16, :].astype(F32)[j:j + 1, :]
                grad = grad + jnp.where(
                    ids == quarter_at + b,
                    gbuf[q, j * BLOCK:(j + 1) * BLOCK, :].astype(F32),
                    0.0,
                )
        part = slice(b * BLOCK, (b + 1) * BLOCK)
        state = to_column(accum[:, part]) + jnp.sum(grad * grad, axis=1, keepdims=True) / width
        o_accum[:, part] = to_row(state)
        fresh = master[part, :] - LR * grad / jnp.sqrt(state)
        o_master[part, :] = fresh
        most = jnp.max(jnp.max(jnp.abs(fresh), axis=0, keepdims=True), axis=1, keepdims=True)
        scale = (most + 1e-6).astype(BF).astype(F32)
        o_srv[g, part, :] = (fresh / scale).astype(BF)
        srows = jnp.where(rows16 == b, scale, srows)
    sbuf[g] = srows.astype(BF)

    def c_copy(k):
        return rcopy(o_srv.at[g], o_srv.at[g], c_s.at[k], c_r.at[k], (grp_peer(k), me))

    def k_copy(k):
        return rcopy(sbuf.at[g], sbuf.at[g], k_s.at[k], k_r.at[k], (grp_peer(k), me))

    for k in range(1, groups):
        c_copy(k).start()
        k_copy(k).start()

    def tc_copy(k):
        to = chip_peer(k)
        return rcopy(t_c.at[to // 2], t_cr.at[k], tc_s.at[k], tc_r.at[k], (g, to))

    total = t_own[pl.ds(pl.multiple_of(g * quarter, quarter), quarter), :]
    for k in range(1, groups):
        tb_copy(k).wait_recv()
        total = total + t_br[k].astype(F32)
    piece = quarter // nz
    for q in range(nz):
        t_c[q] = total[q * piece:(q + 1) * piece, :].astype(t_c.dtype)
    loop(1, nz, lambda k: tc_copy(k).start())

    def gather_piece(k, total):
        tc_copy(k).wait_recv()
        return total + t_cr[k].astype(F32)

    final = lax.fori_loop(1, nz, gather_piece, t_c[z].astype(F32))

    def td_copy(k):
        return rcopy(f_d.at[z], f_d.at[z], td_s.at[k], td_r.at[k], (g, chip_peer(k)))

    f_d[z] = final.astype(BF).astype(f_d.dtype)
    loop(1, nz, lambda k: td_copy(k).start())
    loop(1, nz, lambda k: td_copy(k).wait_recv())

    def te_copy(k):
        return rcopy(f_e.at[g], f_e.at[g], te_s.at[k], te_r.at[k], (grp_peer(k), me))

    def tf_copy(k):
        q = grp_peer(k)
        return rcopy(f_e.at[q], f_f.at[q], tf_s.at[k], tf_r.at[k], (g, pal))

    f_e[g] = f_d[...].reshape(quarter, width).astype(BF)
    for k in range(1, groups):
        te_copy(k).start()
    tf_copy(0).start()
    for k in range(1, groups):
        te_copy(k).wait_recv()

    for k in range(1, groups):
        tf_copy(k).start()

    for k in range(1, groups):
        k_copy(k).wait_recv()
    lane = iota((1, width), 1)
    line = jnp.zeros((1, width), F32)
    for q in range(groups):
        block = sbuf[q].astype(F32)
        for b in range(per):
            line = jnp.where(lane == q * per + b, block[b:b + 1, :], line)
    o_scl[...] = line[:, :groups * per].astype(BF)

    def place_half(ref, at):
        flat = ref[...].reshape(groups * quarter, width).astype(F32)
        for j in range(half // BLOCK):
            column = pl.multiple_of(at * half + j * BLOCK, BLOCK)
            o_top[:, pl.ds(column, BLOCK)] = flat[j * feats:(j + 1) * feats, :]

    place_half(f_e, c)
    for k in range(groups):
        tf_copy(k).wait_recv()
    place_half(f_f, 1 - c)
    for k in range(1, groups):
        c_copy(k).wait_recv()

    a_copy(me, pal, a_s.at[0]).wait_send()

    def left(k):
        a_copy(me, pal, a_s.at[k]).wait_send()
        a_copy(me, pal, a_f.at[k]).wait_send()
        tc_copy(k).wait_send()
        td_copy(k).wait_send()

    loop(1, nz, left)
    loop(1, n, lambda k: h_copy(row_peer(k), me, k).wait_send())
    ta_copy().wait_send()
    for k in range(1, groups):
        g_copy(k).wait_send()
        tb_copy(k).wait_send()
        c_copy(k).wait_send()
        k_copy(k).wait_send()
        te_copy(k).wait_send()
    for k in range(groups):
        tf_copy(k).wait_send()


def on_device(
    n, groups,
    serving, serving_scale, hot_blocks, bag_lengths, bag_indices, dense_act, labels,
    w_top, w_out, master, accum,
):
    rows, width = serving.shape
    blocks = rows // BLOCK
    count = hot_blocks.shape[1]
    span = count * BLOCK
    bags = bag_lengths.shape[1]
    nnz = bag_indices.shape[1]
    cap = nnz // (2 * n)
    capp = -(-cap // 16) * 16
    feats, ff = w_top.shape
    nz = n // 2
    owned = master.shape[1]
    half_rows = feats * ff // 2 // width
    quarter = half_rows // groups
    piece = quarter // nz
    piece_type = BF if piece % 16 == 0 else F32
    vmem = pl.BlockSpec(memory_space=pltpu.VMEM)
    dma = pltpu.SemaphoreType.DMA
    out = pl.pallas_call(
        functools.partial(kernel, (n, groups, cap)),
        out_shape=(
            jax.ShapeDtypeStruct((owned, width), F32),
            jax.ShapeDtypeStruct((1, owned), F32),
            jax.ShapeDtypeStruct((groups, rows // groups, width), BF),
            jax.ShapeDtypeStruct((1, blocks), BF),
            jax.ShapeDtypeStruct((feats, ff), F32),
        ),
        in_specs=[vmem] * 11,
        out_specs=(vmem,) * 5,
        scratch_shapes=[
            pltpu.VMEM((n, span + 16, width), BF),
            pltpu.VMEM((n, bags, span), BF),
            pltpu.VMEM((n, span, bags), BF),
            pltpu.VMEM((n, capp, span), BF),
            pltpu.VMEM((n, capp + 16, width), BF),
            pltpu.VMEM((n, capp + 16, width), BF),
            pltpu.VMEM((groups, span + 16, width), BF),
            pltpu.VMEM((groups, 16, width), BF),
            pltpu.VMEM((bags, width), F32),
            pltpu.VMEM((bags, feats), BF),
            pltpu.VMEM((2, bags, ff // 2), BF),
            pltpu.VMEM((half_rows, width), BF),
            pltpu.VMEM((half_rows, width), F32),
            pltpu.VMEM((half_rows, width), BF),
            pltpu.VMEM((half_rows, width), BF),
            pltpu.VMEM((groups, quarter, width), BF),
            pltpu.VMEM((nz, piece, width), piece_type),
            pltpu.VMEM((nz, piece, width), piece_type),
            pltpu.VMEM((nz, piece, width), piece_type),
            pltpu.VMEM((groups, quarter, width), BF),
            pltpu.VMEM((groups, quarter, width), BF),
            dma((nz,)), dma((nz,)), dma((n,)),
            dma((n,)), dma((n,)),
            dma((groups,)), dma((groups,)),
            dma((groups,)), dma((groups,)),
            dma((groups,)), dma((groups,)),
            dma, dma,
            dma((groups,)), dma((groups,)),
            dma((nz,)), dma((nz,)),
            dma((nz,)), dma((nz,)),
            dma((groups,)), dma((groups,)),
            dma((groups,)), dma((groups,)),
        ],
        compiler_params=pltpu.CompilerParams(
            collective_id=0, has_side_effects=True, vmem_limit_bytes=60 * 2**20
        ),
        name="step",
    )(
        hot_blocks, serving, serving_scale.reshape(1, -1), bag_lengths, bag_indices, dense_act,
        labels.reshape(1, -1), w_top, w_out.reshape(1, -1), master[0], accum,
    )
    new_master, new_accum, fresh, fresh_scale, top = out
    return (new_master[None], new_accum, fresh.reshape(rows, width), fresh_scale[0], top)


def solution(mesh):
    return jax.shard_map(
        functools.partial(on_device, mesh.shape["row"], mesh.shape["grp"]),
        mesh=mesh,
        in_specs=(
            P("row", None),
            P("row"),
            P("grp", "row"),
            P(("grp", "row"), None),
            P(("grp", "row"), None),
            P(("grp", "row"), None),
            P(("grp", "row")),
            P(),
            P(),
            P("grp", "row", None),
            P("grp", "row"),
        ),
        out_specs=(P("grp", "row", None), P("grp", "row"), P("row", None), P("row"), P()),
        check_vma=False,
    )
```

```python
import functools

import jax
import jax.numpy as jnp
from jax import lax
from jax.experimental import pallas as pl
from jax.experimental.pallas import tpu as pltpu
from jax.sharding import PartitionSpec as P

BLOCK = 128
LR = 0.05
MESH = pl.DeviceIdType.MESH
BF = jnp.bfloat16
F32 = jnp.float32


def nt(a, b):
    return lax.dot_general(a, b, (((1,), (1,)), ((), ())), preferred_element_type=F32)


def nn(a, b):
    return jnp.dot(a, b, preferred_element_type=F32)


def tn(a, b):
    return lax.dot_general(a, b, (((0,), (0,)), ((), ())), preferred_element_type=F32)


def iota(shape, axis):
    return lax.broadcasted_iota(jnp.int32, shape, axis)


def to_column(row):
    m = row.shape[1]
    keep = iota((m, m), 0) == iota((m, m), 1)
    return jnp.sum(jnp.where(keep, row, jnp.zeros_like(row)), axis=1, keepdims=True)


def to_row(column):
    m = column.shape[0]
    keep = iota((m, m), 0) == iota((m, m), 1)
    return jnp.sum(jnp.where(keep, column, jnp.zeros_like(column)), axis=0, keepdims=True)


def rcopy(src, dst, send, recv, device):
    return pltpu.make_async_remote_copy(
        src_ref=src, dst_ref=dst, send_sem=send, recv_sem=recv,
        device_id=device, device_id_type=MESH,
    )


def loop(lo, hi, body):
    if hi - lo <= 8:
        for k in range(lo, hi):
            body(k)
        return

    def step(k, carry):
        body(k)
        return carry

    lax.fori_loop(lo, hi, step, 0)


def kernel(
    dims,
    hot, srv, scl, lens, idx, dense, labels, w_top, w_out, master, accum,
    o_master, o_accum, o_srv, o_scl, o_top,
    tbl, cnt, few, hmsg, hrecv, gbuf, sbuf, pooled, joined, dpre,
    t_rows, t_sum, t_send, t_own, t_a, t_b, t_br, t_c, t_cr, f_d, f_e, f_f,
    a_s, a_f, a_r, h_s, h_r, g_s, g_r, c_s, c_r, k_s, k_r,
    ta_s, ta_r, tb_s, tb_r, tc_s, tc_r, td_s, td_r, te_s, te_r, tf_s, tf_r,
):
    n, groups, cap = dims
    nz = n // 2
    g = lax.axis_index("grp")
    me = lax.axis_index("row")
    z, c = me // 2, me % 2
    pal = z * 2 + (1 - c)
    count = hot.shape[1]
    span = count * BLOCK
    capp = hmsg.shape[1] - 16
    bags = lens.shape[1]
    nnz = idx.shape[1]
    width = srv.shape[1]
    per = master.shape[0] // BLOCK
    ff = w_top.shape[1]
    half = ff // 2

    def row_peer(k):
        return (me + k) % n

    def chip_peer(k):
        return ((z + k) % nz) * 2 + c

    def grp_peer(k):
        return (g + k) % groups

    barrier = pltpu.get_barrier_semaphore()

    def greet(k):
        pl.semaphore_signal(barrier, inc=1, device_id=(g, row_peer(k)), device_id_type=MESH)

    loop(1, n, greet)
    for k in range(1, groups):
        pl.semaphore_signal(barrier, inc=1, device_id=(grp_peer(k), me), device_id_type=MESH)

    lane_b = iota((1, scl.shape[1]), 1)
    scales = scl[...].astype(F32)
    rows16 = iota((16, width), 0)
    scale_rows = jnp.zeros((16, width), F32)
    id_rows = jnp.zeros((16, width), F32)
    for j in range(count):
        block = hot[:, j:j + 1]
        one = jnp.sum(jnp.where(lane_b == block, scales, 0.0), axis=1, keepdims=True)
        scale_rows = jnp.where(rows16 == j, one, scale_rows)
        id_rows = jnp.where(rows16 == j, block.astype(F32), id_rows)
        chosen = jnp.broadcast_to(block, (8, width))
        rows = jnp.zeros((BLOCK, width), F32)
        for b in range(scl.shape[1]):
            mask = jnp.where(chosen == b, 1.0, 0.0)[0:1, :]
            rows = rows + srv[b * BLOCK:(b + 1) * BLOCK, :].astype(F32) * mask
        tbl[me, j * BLOCK:(j + 1) * BLOCK, :] = rows.astype(BF)
    tbl[me, span:span + 16, :] = scale_rows.astype(BF)
    gbuf[g, span:span + 16, :] = id_rows.astype(BF)

    pl.semaphore_wait(barrier, n - 1 + groups - 1)

    def a_copy(source, to, send):
        return rcopy(tbl.at[source], tbl.at[source], send, a_r.at[source], (g, to))

    loop(1, nz, lambda k: a_copy(me, chip_peer(k), a_s.at[k]).start())
    a_copy(me, pal, a_s.at[0]).start()

    lengths = lens[...]
    tri = iota((bags, bags), 1) <= iota((bags, bags), 0)
    ends = jnp.sum(jnp.where(tri, lengths, 0), axis=1, keepdims=True)
    starts = ends - to_column(lengths)
    place = iota((bags, nnz), 1)
    in_bag = jnp.where((place >= starts) & (place < ends), 1.0, 0.0).astype(BF)
    indices = idx[...]
    upper = jnp.where(iota((span, span), 0) <= iota((span, span), 1), 1.0, 0.0).astype(BF)
    numbers = iota((8, span), 1).astype(F32).astype(BF)

    def count_range(r):
        which = jnp.where(indices - r * span == iota((span, nnz), 0), 1.0, 0.0).astype(BF)
        counts = nt(in_bag, which)
        whole = counts.astype(BF)
        cnt[r] = whole
        used = jnp.where(jnp.sum(counts, axis=0, keepdims=True) > 0.0, 1.0, 0.0)
        rank = nn(jnp.broadcast_to(used, (8, span)).astype(BF), upper)[0:1, :]
        order = jnp.where(used > 0.0, rank.astype(jnp.int32) - 1, -1)
        picked = jnp.where(iota((width, span), 0) == order, 1.0, 0.0).astype(BF)
        few[r] = nt(picked[:capp, :], whole).astype(BF)
        hmsg[r, capp:capp + 16, :] = jnp.concatenate(
            [nt(numbers, picked), jnp.zeros((8, width), F32)], axis=0
        ).astype(BF)

    loop(0, n, count_range)

    joined[:, width:] = dense[...]

    def pool(r):
        block_scale = tbl[r, span:span + 16, :].astype(F32)
        total = pooled[...]
        for j in range(count):
            part = slice(j * BLOCK, (j + 1) * BLOCK)
            total = total + nn(cnt[r, :, part], tbl[r, part, :]) * block_scale[j:j + 1, :]
        pooled[...] = total

    pooled[...] = jnp.zeros_like(pooled)
    pool(me)

    def relay(k):
        source = chip_peer(k)
        a_copy(source, source, a_f.at[k]).wait_recv()
        a_copy(source, pal, a_f.at[k]).start()
        pool(source)

    loop(1, nz, relay)

    def other(k):
        source = ((z + k) % nz) * 2 + (1 - c)
        a_copy(source, pal, a_f.at[0]).wait_recv()
        pool(source)

    loop(0, nz, other)
    joined[:, :width] = pooled[...].astype(BF)

    pre = nn(joined[...], w_top[...])
    sig = jax.nn.sigmoid(pre)
    out_w = w_out[...]
    logit = jnp.sum(pre * sig * out_w, axis=1, keepdims=True)
    dlogit = jax.nn.sigmoid(logit) - to_column(labels[...])
    dp = (dlogit * out_w * (sig * (1.0 + pre * (1.0 - sig)))).astype(BF)
    dpre[0] = dp[:, :half]
    dpre[1] = dp[:, half:]
    dz = nt(dp, w_top[:width, :]).astype(BF)

    def ta_copy():
        return rcopy(t_send, t_a, ta_s, ta_r, (g, pal))

    feats = w_top.shape[0]
    theirs = tn(joined[...], dpre[1 - c])
    for j in range(half // BLOCK):
        t_send[j * feats:(j + 1) * feats, :] = theirs[:, j * BLOCK:(j + 1) * BLOCK].astype(BF)
    ta_copy().start()

    def h_copy(to, source, k):
        return rcopy(hmsg.at[to], hrecv.at[source], h_s.at[k], h_r.at[source], (g, to))

    def spread(r):
        hmsg[r, :capp, :] = nn(few[r], dz).astype(BF)

    loop(0, n, spread)
    loop(1, n, lambda k: h_copy(row_peer(k), me, k).start())

    mine = tn(joined[...], dpre[c])
    for j in range(half // BLOCK):
        t_own[j * feats:(j + 1) * feats, :] = mine[:, j * BLOCK:(j + 1) * BLOCK]

    quarter = t_own.shape[0] // groups

    def part_of(ref, q):
        return ref.at[pl.ds(pl.multiple_of(q * quarter, quarter), quarter)]

    def tb_copy(k):
        return rcopy(
            part_of(t_b, grp_peer(k)), t_br.at[k], tb_s.at[k], tb_r.at[k], (grp_peer(k), me)
        )

    ta_copy().wait_recv()
    both = t_own[...] + t_a[...].astype(F32)
    t_own[...] = both
    t_b[...] = both.astype(BF)
    for k in range(1, groups):
        tb_copy(k).start()

    def g_copy(k):
        return rcopy(gbuf.at[g], gbuf.at[g], g_s.at[k], g_r.at[k], (grp_peer(k), me))

    def expand(message):
        place_of = message[capp:capp + 1, :].astype(F32)
        put = jnp.where(
            iota((span, width), 0).astype(F32) == place_of, 1.0, 0.0
        ).astype(BF)
        return nn(put[:, :capp], message[:capp, :])

    t_rows[...] = expand(hmsg[me])

    def arrive(k):
        source = row_peer(k)
        h_copy(source, source, k).wait_recv()
        t_rows[...] += expand(hrecv[source])

    loop(1, n, arrive)
    gbuf[g, :span, :] = t_rows[...].astype(BF)
    for k in range(1, groups):
        g_copy(k).start()

    def tc_copy(k):
        to = chip_peer(k)
        return rcopy(t_c.at[to // 2], t_cr.at[k], tc_s.at[k], tc_r.at[k], (g, to))

    total = t_own[pl.ds(pl.multiple_of(g * quarter, quarter), quarter), :]
    for k in range(1, groups):
        tb_copy(k).wait_recv()
        total = total + t_br[k].astype(F32)
    piece = quarter // nz
    for q in range(nz):
        t_c[q] = total[q * piece:(q + 1) * piece, :].astype(t_c.dtype)
    loop(1, nz, lambda k: tc_copy(k).start())

    t_sum[...] = t_c[z].astype(F32)

    def gather_piece(k):
        tc_copy(k).wait_recv()
        t_sum[...] += t_cr[k].astype(F32)

    loop(1, nz, gather_piece)

    def td_copy(k):
        return rcopy(f_d.at[z], f_d.at[z], td_s.at[k], td_r.at[k], (g, chip_peer(k)))

    f_d[z] = t_sum[...].astype(BF).astype(f_d.dtype)
    loop(1, nz, lambda k: td_copy(k).start())

    for k in range(1, groups):
        g_copy(k).wait_recv()
    srows = jnp.zeros((16, width), F32)
    quarter_at = (g * per).astype(F32)
    for b in range(per):
        grad = jnp.zeros((BLOCK, width), F32)
        for q in range(groups):
            for j in range(count):
                ids = gbuf[q, span:span + 16, :].astype(F32)[j:j + 1, :]
                grad = grad + jnp.where(
                    ids == quarter_at + b,
                    gbuf[q, j * BLOCK:(j + 1) * BLOCK, :].astype(F32),
                    0.0,
                )
        part = slice(b * BLOCK, (b + 1) * BLOCK)
        state = to_column(accum[:, part]) + jnp.sum(grad * grad, axis=1, keepdims=True) / width
        o_accum[:, part] = to_row(state)
        fresh = master[part, :] - LR * grad / jnp.sqrt(state)
        o_master[part, :] = fresh
        most = jnp.max(jnp.max(jnp.abs(fresh), axis=0, keepdims=True), axis=1, keepdims=True)
        scale = (most + 1e-6).astype(BF).astype(F32)
        o_srv[g, part, :] = (fresh / scale).astype(BF)
        srows = jnp.where(rows16 == b, scale, srows)
    sbuf[g] = srows.astype(BF)

    def c_copy(k):
        return rcopy(o_srv.at[g], o_srv.at[g], c_s.at[k], c_r.at[k], (grp_peer(k), me))

    def k_copy(k):
        return rcopy(sbuf.at[g], sbuf.at[g], k_s.at[k], k_r.at[k], (grp_peer(k), me))

    for k in range(1, groups):
        c_copy(k).start()
        k_copy(k).start()

    loop(1, nz, lambda k: td_copy(k).wait_recv())

    def te_copy(k):
        return rcopy(f_e.at[g], f_e.at[g], te_s.at[k], te_r.at[k], (grp_peer(k), me))

    def tf_copy(k):
        q = grp_peer(k)
        return rcopy(f_e.at[q], f_f.at[q], tf_s.at[k], tf_r.at[k], (g, pal))

    f_e[g] = f_d[...].reshape(quarter, width).astype(BF)
    for k in range(1, groups):
        te_copy(k).start()
    tf_copy(0).start()
    for k in range(1, groups):
        te_copy(k).wait_recv()

    for k in range(1, groups):
        tf_copy(k).start()

    for k in range(1, groups):
        k_copy(k).wait_recv()
    lane = iota((1, width), 1)
    line = jnp.zeros((1, width), F32)
    for q in range(groups):
        block = sbuf[q].astype(F32)
        for b in range(per):
            line = jnp.where(lane == q * per + b, block[b:b + 1, :], line)
    o_scl[...] = line[:, :groups * per].astype(BF)

    def place_half(ref, at):
        flat = ref[...].reshape(groups * quarter, width)
        for j in range(half // BLOCK):
            column = pl.multiple_of(at * half + j * BLOCK, BLOCK)
            o_top[:, pl.ds(column, BLOCK)] = flat[j * feats:(j + 1) * feats, :]

    place_half(f_e, c)

    for k in range(groups):
        tf_copy(k).wait_recv()
    place_half(f_f, 1 - c)
    for k in range(1, groups):
        c_copy(k).wait_recv()

    a_copy(me, pal, a_s.at[0]).wait_send()

    def left(k):
        a_copy(me, pal, a_s.at[k]).wait_send()
        a_copy(me, pal, a_f.at[k]).wait_send()
        tc_copy(k).wait_send()
        td_copy(k).wait_send()

    loop(1, nz, left)
    loop(1, n, lambda k: h_copy(row_peer(k), me, k).wait_send())
    ta_copy().wait_send()
    for k in range(1, groups):
        g_copy(k).wait_send()
        tb_copy(k).wait_send()
        c_copy(k).wait_send()
        k_copy(k).wait_send()
        te_copy(k).wait_send()
    for k in range(groups):
        tf_copy(k).wait_send()


def write_out(*refs):
    for source, target in zip(refs[:5], refs[5:]):
        target[...] = source[...].astype(target.dtype)


def on_device(
    n, groups,
    serving, serving_scale, hot_blocks, bag_lengths, bag_indices, dense_act, labels,
    w_top, w_out, master, accum,
):
    rows, width = serving.shape
    blocks = rows // BLOCK
    count = hot_blocks.shape[1]
    span = count * BLOCK
    bags = bag_lengths.shape[1]
    nnz = bag_indices.shape[1]
    cap = nnz // (2 * n)
    capp = -(-cap // 16) * 16
    feats, ff = w_top.shape
    nz = n // 2
    owned = master.shape[1]
    half_rows = feats * ff // 2 // width
    quarter = half_rows // groups
    piece = quarter // nz
    piece_type = BF if piece % 16 == 0 else F32
    vmem = pl.BlockSpec(memory_space=pltpu.VMEM)
    dma = pltpu.SemaphoreType.DMA
    out = pl.pallas_call(
        functools.partial(kernel, (n, groups, cap)),
        out_shape=(
            jax.ShapeDtypeStruct((owned, width), F32),
            jax.ShapeDtypeStruct((1, owned), F32),
            jax.ShapeDtypeStruct((groups, rows // groups, width), BF),
            jax.ShapeDtypeStruct((1, blocks), BF),
            jax.ShapeDtypeStruct((feats, ff), BF),
        ),
        in_specs=[vmem] * 11,
        out_specs=(vmem,) * 5,
        scratch_shapes=[
            pltpu.VMEM((n, span + 16, width), BF),
            pltpu.VMEM((n, bags, span), BF),
            pltpu.VMEM((n, capp, bags), BF),
            pltpu.VMEM((n, capp + 16, width), BF),
            pltpu.VMEM((n, capp + 16, width), BF),
            pltpu.VMEM((groups, span + 16, width), BF),
            pltpu.VMEM((groups, 16, width), BF),
            pltpu.VMEM((bags, width), F32),
            pltpu.VMEM((bags, feats), BF),
            pltpu.VMEM((2, bags, ff // 2), BF),
            pltpu.VMEM((span, width), F32),
            pltpu.VMEM((piece, width), F32),
            pltpu.VMEM((half_rows, width), BF),
            pltpu.VMEM((half_rows, width), F32),
            pltpu.VMEM((half_rows, width), BF),
            pltpu.VMEM((half_rows, width), BF),
            pltpu.VMEM((groups, quarter, width), BF),
            pltpu.VMEM((nz, piece, width), piece_type),
            pltpu.VMEM((nz, piece, width), piece_type),
            pltpu.VMEM((nz, piece, width), piece_type),
            pltpu.VMEM((groups, quarter, width), BF),
            pltpu.VMEM((groups, quarter, width), BF),
            dma((nz,)), dma((nz,)), dma((n,)),
            dma((n,)), dma((n,)),
            dma((groups,)), dma((groups,)),
            dma((groups,)), dma((groups,)),
            dma((groups,)), dma((groups,)),
            dma, dma,
            dma((groups,)), dma((groups,)),
            dma((nz,)), dma((nz,)),
            dma((nz,)), dma((nz,)),
            dma((groups,)), dma((groups,)),
            dma((groups,)), dma((groups,)),
        ],
        compiler_params=pltpu.CompilerParams(
            collective_id=0, has_side_effects=True, vmem_limit_bytes=60 * 2**20
        ),
        name="step",
    )(
        hot_blocks, serving, serving_scale.reshape(1, -1), bag_lengths, bag_indices, dense_act,
        labels.reshape(1, -1), w_top, w_out.reshape(1, -1), master[0], accum,
    )
    new_master, new_accum, fresh, fresh_scale, top = pl.pallas_call(
        write_out,
        out_shape=(
            jax.ShapeDtypeStruct((owned, width), F32),
            jax.ShapeDtypeStruct((1, owned), F32),
            jax.ShapeDtypeStruct((rows, width), BF),
            jax.ShapeDtypeStruct((1, blocks), BF),
            jax.ShapeDtypeStruct((feats, ff), F32),
        ),
        in_specs=[vmem] * 5,
        out_specs=(vmem,) * 5,
        name="write",
    )(out[0], out[1], out[2].reshape(rows, width), out[3], out[4])
    return (new_master[None], new_accum, fresh, fresh_scale[0], top)


def solution(mesh):
    return jax.shard_map(
        functools.partial(on_device, mesh.shape["row"], mesh.shape["grp"]),
        mesh=mesh,
        in_specs=(
            P("row", None),
            P("row"),
            P("grp", "row"),
            P(("grp", "row"), None),
            P(("grp", "row"), None),
            P(("grp", "row"), None),
            P(("grp", "row")),
            P(),
            P(),
            P("grp", "row", None),
            P("grp", "row"),
        ),
        out_specs=(P("grp", "row", None), P("grp", "row"), P("row", None), P("row"), P()),
        check_vma=False,
    )
```
